1024 devices in a mesh: dp: 16 (over x, y_lo), mp: 64 (over z, y_hi, core).
Axes of the slice: x: 4, y: 8 (y_hi: 2, y_lo: 4; y = y_hi * 4 + y_lo), z: 16, core: 2. Of those that a mesh axis runs over, the one named last changes fastest.
Arguments:
- tokens: bfloat16 [2048, 6144], P(('dp', 'mp')), may hold values from -6 to 6
- norm_gain: float32 [6144], replicated, may hold values from 0.5 to 1.5
- up_weight: bfloat16 [6144, 16384], P(None, 'mp'), may hold values from -0.078125 to 0.078125
- down_weight: bfloat16 [16384, 6144], P('mp'), may hold values from -0.046875 to 0.046875
- out_grad: bfloat16 [2048, 6144], P(('dp', 'mp')), may hold values from -6 to 6
Outputs:
- input_grad: bfloat16 [2048, 6144], P(('dp', 'mp'))
- up_grad: bfloat16 [6144, 16384], P('dp', 'mp')
- down_grad: bfloat16 [16384, 6144], P('mp', 'dp')
- gain_grad: float32 [6144], replicated
The draws below stay inside these ranges and needn't reach their ends.
All inputs are finite; a program needn't handle non-finite values.
Results may differ from the reference program's by a relative error of at most 0.018.
Values may be sent and summed in bfloat16 or wider, within the bound.
A program may use at most 64 MiB of HBM per device.

```python
import math
import jax
import jax.numpy as jnp
from jax import lax

D = 6144
FF_WIN = 16384
TOK_GROUP = 128
TOKENS = 2048
N_DP = 16


def block_levels(key, dims, split, least, high):
    def one(position, blocks):
        heights = jax.random.uniform(jax.random.fold_in(jax.random.fold_in(key, 6), position), (blocks,), jnp.float32, least / len(split), high / len(split))
        return jnp.repeat(jnp.exp(heights), dims[position] // blocks).reshape((-1,) + (1,) * (len(dims) - position - 1))

    loudness = one(*split[0])
    for cut in split[1:]:
        loudness = loudness * one(*cut)
    return loudness


def bell_draw(key, shape, deviation, bound, cuts=(), kind=jnp.bfloat16):
    result = deviation * jax.random.normal(key, shape, jnp.float32)
    if cuts:
        result = result * block_levels(key, shape, cuts, -0.22, 0.18)
    return jnp.clip(result, -bound, bound).astype(kind)


def setup_inputs(seed: int = 0) -> dict:
    arg_keys = jax.random.split(jax.random.key(seed), 6)
    tokens = bell_draw(arg_keys[0], (TOKENS, D), 1.0, 6.0, ((0, 1024),))
    norm_gain = jnp.clip(1.0 + 0.1 * jax.random.normal(arg_keys[1], (D,), jnp.float32), 0.5, 1.5)
    up_weight = bell_draw(arg_keys[2], (D, FF_WIN), D ** -0.5, 0.078125, ((1, 64),))
    down_weight = bell_draw(arg_keys[3], (FF_WIN, D), FF_WIN ** -0.5, 0.046875, ((0, 64),))
    out_grad = bell_draw(arg_keys[4], (TOKENS, D), 1.0, 6.0, ((0, 1024),))
    return dict(tokens=tokens, norm_gain=norm_gain, up_weight=up_weight, down_weight=down_weight, out_grad=out_grad)


def gelu_value(preact):
    return 0.5 * preact * (1.0 + lax.erf(preact * 0.7071067811865476))

def gelu_slope(preact):
    return 0.5 * (1.0 + lax.erf(preact * 0.7071067811865476)) + preact * jnp.exp(-0.5 * preact * preact) * 0.3989422804014327

def reference(tokens, norm_gain, up_weight, down_weight, out_grad):
    values = tokens.astype(jnp.float32)
    centered = values - lax.optimization_barrier(jnp.mean(values, axis=1, keepdims=True))
    inv_std = lax.rsqrt(lax.optimization_barrier(jnp.mean(centered * centered, axis=1, keepdims=True)) + 1e-06)
    x_hat = centered * inv_std
    normed = (x_hat * norm_gain).astype(jnp.bfloat16)
    preact = jnp.dot(normed, up_weight, preferred_element_type=jnp.float32)
    hidden = gelu_value(preact).astype(jnp.bfloat16)
    hid_grad = jnp.dot(out_grad, down_weight.T, preferred_element_type=jnp.float32)
    pre_grad = (hid_grad * gelu_slope(preact)).astype(jnp.bfloat16)
    norm_grad = jnp.dot(pre_grad, up_weight.T, preferred_element_type=jnp.float32)
    factor = 1.0 / math.sqrt(TOKENS)
    gain_grad = lax.optimization_barrier(jnp.sum(norm_grad * x_hat, axis=0)) * factor
    scaled = norm_gain * norm_grad
    input_grad = (scaled - lax.optimization_barrier(jnp.mean(scaled, axis=1, keepdims=True)) - x_hat * lax.optimization_barrier(jnp.mean(scaled * x_hat, axis=1, keepdims=True))) * inv_std
    up_total = jnp.zeros((D, FF_WIN), jnp.float32)
    down_total = jnp.zeros((FF_WIN, D), jnp.float32)
    for replica in range(N_DP):
        first = replica * TOK_GROUP
        last = first + TOK_GROUP
        up_part = jnp.dot(normed[first:last].T, pre_grad[first:last], preferred_element_type=jnp.float32)
        down_part = jnp.dot(hidden[first:last].T, out_grad[first:last], preferred_element_type=jnp.float32)
        up_total = up_total + up_part.astype(jnp.bfloat16).astype(jnp.float32)
        down_total = down_total + down_part.astype(jnp.bfloat16).astype(jnp.float32)
    up_grad = (up_total * factor).astype(jnp.bfloat16)
    down_grad = (down_total * factor).astype(jnp.bfloat16)
    return (input_grad.astype(jnp.bfloat16), up_grad, down_grad, gain_grad)
```

```python
import functools
import math

import jax
import jax.numpy as jnp
from jax import lax
from jax.experimental import pallas as pl
from jax.experimental.pallas import tpu as pltpu
from jax.sharding import Mesh
from jax.sharding import PartitionSpec as P

MP = ("mp_0", "mp_1", "mp_2")
DP = ("dp_0", "dp_1")
DP_MP = ("dp_0", "dp_1", "mp_0", "mp_1", "mp_2")
MESH = pl.DeviceIdType.MESH
GATHER_CUTS = 2
SUM_CUTS = 2
VMEM = pl.BlockSpec(memory_space=pltpu.VMEM)


def place():
    x, y_lo = lax.axis_index("dp_0"), lax.axis_index("dp_1")
    z, y_hi, core = (lax.axis_index(a) for a in MP)
    return x, y_lo, z, y_hi, core


def at_y(y):
    y = lax.rem(y, 8)
    return {"dp_1": lax.rem(y, 4), "mp_1": lax.div(y, 4)}


def remote(src, dst, send, recv, to):
    return pltpu.make_async_remote_copy(
        src_ref=src, dst_ref=dst, send_sem=send, recv_sem=recv, device_id=to, device_id_type=MESH
    )


def await_bytes(ref, sem):
    pltpu.make_async_copy(ref, ref, sem).wait()


def greet(to):
    pl.semaphore_signal(pltpu.get_barrier_semaphore(), inc=1, device_id=to, device_id_type=MESH)


def normalised(tokens):
    values = tokens.astype(jnp.float32)
    centered = values - jnp.mean(values, axis=1, keepdims=True)
    inv_std = lax.rsqrt(jnp.mean(centered * centered, axis=1, keepdims=True) + 1e-06)
    return centered * inv_std, inv_std


def gather_kernel(
    tok, cot, gain, ring, other, cols, mine, stage, tile,
    pair_send, pair_recv, send_r, send_l, recv_l, recv_r, side_send, side_recv, cols_send, cols_recv,
):
    x, y_lo, z, y_hi, core = place()
    slots, _, width = ring.shape
    half = slots // 2
    block = cols.shape[3]
    cuts = GATHER_CUTS
    cut = width // cuts
    y = y_hi * 4 + y_lo
    which = lax.rem(y_hi + core, 2)
    dp = x * 4 + y_lo
    right, left = lax.rem(z + 1, slots), lax.rem(z + slots - 1, slots)
    flip_y, flip_core = 1 - y_hi, 1 - core

    def steps_y(turn):
        return (0, 1, 7, 2 + 4 * which)[turn]

    for to in (
        {"mp_2": flip_core},
        {"mp_1": flip_y},
        {"mp_1": flip_y, "mp_2": flip_core},
        {"mp_0": right},
        {"mp_0": left},
    ):
        greet(to)
    for turn in range(4):
        def hello(dx, _, turn=turn):
            there = at_y(y + 8 - steps_y(turn))
            greet({"dp_0": lax.rem(x + 4 - dx, 4), **there, "mp_2": lax.rem(which + there["mp_1"], 2)})
            return 0
        lax.fori_loop(1 if turn == 0 else 0, 4, hello, 0)

    x_hat, _ = normalised(tok[...])
    mine[0] = (x_hat * gain[...]).astype(jnp.bfloat16)
    mine[1] = cot[...]

    pl.semaphore_wait(pltpu.get_barrier_semaphore(), 20)

    first = remote(mine, stage.at[0], pair_send.at[0], pair_recv.at[0], {"mp_1": flip_y, "mp_2": flip_core})
    across = remote(mine, stage.at[1], pair_send.at[0], pair_recv.at[1], {"mp_1": flip_y})
    beside = remote(mine, stage.at[1], pair_send.at[1], pair_recv.at[1], {"mp_2": flip_core})

    @pl.when(core == 0)
    def _():
        first.start()
        stage[0] = mine[...]

    @pl.when(core == 1)
    def _():
        beside.start()
        across.start()
        first.wait_recv()

    across.wait_recv()
    for kind in range(2):
        @pl.when(which == kind)
        def _(kind=kind):
            for t in range(2):
                for k in range(2):
                    tile[pl.ds(((t + kind) % 2) * 4 + 2 * k, 2), :] = stage[k, t].astype(jnp.float32)
    ring[0] = tile[...].astype(jnp.bfloat16)

    def part(slot, q):
        return ring.at[slot, :, pl.ds(q * cut, cut)]

    def hop_right(s, q):
        return remote(part(s, q), part(s + 1, q), send_r.at[s, q], recv_l.at[s, q], {"mp_0": right})

    def hop_left(s, q):
        here = (slots - s) % slots
        return remote(part(here, q), part(slots - s - 1, q), send_l.at[s, q], recv_r.at[s, q], {"mp_0": left})

    def pass_on(slot):
        remote(ring.at[slot], other.at[slot], side_send, side_recv, {"mp_2": flip_core}).start()

    def spread(lo, n):
        for turn in range(4):
            def to_column(dx, _, turn=turn):
                there = at_y(y + steps_y(turn))
                x_to = lax.rem(x + dx, 4)
                start = pl.multiple_of((x_to * 4 + there["dp_1"]) * block, 128)
                remote(
                    ring.at[pl.ds(lo, n), :, pl.ds(start, block)],
                    cols.at[dp, pl.ds(lo, n)],
                    cols_send,
                    cols_recv,
                    {"dp_0": x_to, **there, "mp_2": lax.rem(which + there["mp_1"], 2)},
                ).start()
                return 0
            lax.fori_loop(1 if turn == 0 else 0, 4, to_column, 0)

    goes_r = lambda s, q: s + 1 < half or q < cuts // 2
    goes_l = lambda s, q: s + 1 < half or q >= cuts // 2
    for s in range(half + 1):
        for q in range(cuts):
            if s > 0 and goes_r(s - 1, q):
                hop_right(s - 1, q).wait_recv()
            if s < half and goes_r(s, q):
                hop_right(s, q).start()
            if s > 0 and goes_l(s - 1, q):
                hop_left(s - 1, q).wait_recv()
            if s < half and goes_l(s, q):
                hop_left(s, q).start()
        pass_on(s)
        if 0 < s < half:
            pass_on(slots - s)
        if s == 2:
            spread(0, 3)
            spread(slots - 2, 2)
        elif s == half:
            spread(s - 1, 3)
        elif s > 2 and s % 2 == 0:
            spread(s - 1, 2)
            spread(slots - s, 2)
    cols[dp] = ring[:, :, pl.ds(pl.multiple_of(dp * block, 128), block)]

    for s in range(half):
        for q in range(cuts):
            if goes_r(s, q):
                hop_right(s, q).wait_send()
            if goes_l(s, q):
                hop_left(s, q).wait_send()

    first.wait_send()

    @pl.when(core == 1)
    def _():
        beside.wait_send()

    await_bytes(other, side_recv)
    await_bytes(ring, side_send)
    most = cols.at[pl.ds(0, cols.shape[0] - 1)]
    await_bytes(most, cols_recv)
    await_bytes(most, cols_send)


def gather_rows(tokens, out_grad, gain, slots, replicas):
    width = tokens.shape[1]
    rows = jax.ShapeDtypeStruct((slots, 8, width), jnp.bfloat16)
    cols = jax.ShapeDtypeStruct((replicas, slots, 8, width // replicas), jnp.bfloat16)
    dma = pltpu.SemaphoreType.DMA
    hops = (slots // 2, GATHER_CUTS)
    return pl.pallas_call(
        gather_kernel,
        name="gather_rows",
        out_shape=(rows, rows, cols),
        in_specs=[VMEM] * 3,
        out_specs=[VMEM] * 3,
        scratch_shapes=[
            pltpu.VMEM((2, 2, width), jnp.bfloat16),
            pltpu.VMEM((2, 2, 2, width), jnp.bfloat16),
            pltpu.VMEM((8, width), jnp.float32),
            dma((2,)), dma((2,)), dma(hops), dma(hops), dma(hops), dma(hops), dma, dma, dma, dma,
        ],
        compiler_params=pltpu.CompilerParams(collective_id=1, has_side_effects=True),
    )(tokens, out_grad, gain)


def exchange_kernel(
    ng, pgh, gp, cols, out_ng, pgh_all, out_gain, other_cols,
    side, go_l, go_r, in_l, in_r, give, take, g1, g2, g3, h1, h2,
    side_send, side_recv, cols_send, cols_recv, send_l, recv_l, send_r, recv_r,
    give_send, take_recv, all_send, all_recv, gain_send, gain_recv,
):
    x, y_lo, z, y_hi, core = place()
    slots, _, width = ng.shape
    half = slots // 2
    part = width // 2
    cuts = SUM_CUTS
    cut = part // cuts
    dp = x * 4 + y_lo
    me = y_hi * 2 + core
    right, left = lax.rem(z + 1, slots), lax.rem(z + slots - 1, slots)
    flip_core = 1 - core

    def dp_peer(k):
        there = lax.rem(dp + k, 16)
        return there, {"dp_0": lax.div(there, 4), "dp_1": lax.rem(there, 4)}

    def quad_peer(k):
        there = lax.rem(me + k, 4)
        return there, {"mp_1": lax.div(there, 2), "mp_2": lax.rem(there, 2)}

    def z_peer(k):
        there = lax.rem(z + k, slots)
        return there, {"mp_0": there}

    for peer, n in ((z_peer, slots), (dp_peer, 16), (quad_peer, 4)):
        lax.fori_loop(1, n, lambda k, _, peer=peer: (greet(peer(k)[1]), 0)[1], 0)
    pl.semaphore_wait(pltpu.get_barrier_semaphore(), slots - 1 + 15 + 3)

    away = pl.multiple_of(flip_core * part, 128)
    home = pl.multiple_of(core * part, 128)
    pieces = ((half - 2, 5), (half - 5, 3), (half + 3, 3), (0, half - 5), (half + 6, slots - half - 6))

    def beside(i):
        lo, n = pieces[i]
        return remote(
            ng.at[pl.ds(lo, n), :, pl.ds(away, part)], side.at[pl.ds(lo, n)], side_send.at[i], side_recv.at[i],
            {"mp_2": flip_core},
        )

    beside(0).start()

    def piece_to(x_from, y_from, to, src=None):
        slot = x_from * 4 + y_from
        here = pgh_all.at[slot] if src is None else src
        return remote(here, pgh_all.at[slot], all_send, all_recv.at[slot], to)

    x_up, x_down = lax.rem(x + 1, 4), lax.rem(x + 3, 4)
    forward = lax.rem(x + 1 + 2 * core, 4)
    behind = lax.rem(x + 3 + 2 * core, 4)
    far = lax.rem(x + 2, 4)

    piece_to(x, y_lo, {"dp_0": x_up}, pgh).start()
    piece_to(x, y_lo, {"dp_0": x_down}, pgh).start()
    for k in range(1, 4):
        piece_to(x, y_lo, {"dp_1": lax.rem(y_lo + k, 4)}, pgh).start()

    def gain_hop(peer, n, src, dst, slot, stage):
        def send(k, _):
            there, to = peer(k)
            remote(src(there), dst.at[slot], gain_send.at[stage], gain_recv.at[stage], to).start()
            return 0
        lax.fori_loop(1, n, send, 0)

    def gain_end(dst, n, stage):
        await_bytes(dst.at[pl.ds(0, n - 1)], gain_recv.at[stage])

    def total(ref, n):
        acc = ref[0]
        for k in range(1, n):
            acc = acc + ref[k]
        return acc

    gain_hop(dp_peer, 16, lambda there: gp.at[there], g1, dp, 0)
    g1[dp] = gp[dp]
    for i in range(1, len(pieces)):
        beside(i).start()
    to_side = remote(cols, other_cols, cols_send, cols_recv, {"mp_2": flip_core})
    to_side.start()
    pgh_all[dp] = pgh[...]

    def own(slot, q):
        here = ng[slot, :, pl.ds(pl.multiple_of(home + q * cut, 128), cut)]
        return here.astype(jnp.float32) + side[slot, :, pl.ds(q * cut, cut)].astype(jnp.float32)

    def hop_l(t, q):
        at = (t, slice(None), pl.ds(q * cut, cut))
        return remote(go_l.at[at], in_l.at[at], send_l.at[t, q], recv_l.at[t, q], {"mp_0": left})

    def hop_r(t, q):
        at = (t, slice(None), pl.ds(q * cut, cut))
        return remote(go_r.at[at], in_r.at[at], send_r.at[t, q], recv_r.at[t, q], {"mp_0": right})

    goes_l = lambda t, q: t > 0 or q < cuts // 2
    goes_r = lambda t, q: t > 0 or q >= cuts // 2
    needed = {0: (0,), 3: (1, 2), 6: (3, 4)}

    for t in range(half):
        for i in needed.get(t, ()):
            beside(i).wait_recv()
        for q in range(cuts):
            cols_q = pl.ds(q * cut, cut)
            if goes_l(t, q):
                value = own(half - t, q)
                if t > 0 and goes_l(t - 1, q):
                    hop_l(t - 1, q).wait_recv()
                    value = value + in_l[t - 1, :, cols_q].astype(jnp.float32)
                go_l[t, :, cols_q] = value.astype(jnp.bfloat16)
                hop_l(t, q).start()
            if goes_r(t, q):
                value = own(half + t, q)
                if t > 0 and goes_r(t - 1, q):
                    hop_r(t - 1, q).wait_recv()
                    value = value + in_r[t - 1, :, cols_q].astype(jnp.float32)
                go_r[t, :, cols_q] = value.astype(jnp.bfloat16)
                hop_r(t, q).start()
        if t == 1:
            piece_to(behind, y_lo, {"dp_0": forward}).wait_recv()
            piece_to(behind, y_lo, {"dp_0": forward}).start()
            gain_end(g1, 16, 0)
            h1[...] = total(g1, 16)
            g2[me] = h1[...]
            gain_hop(quad_peer, 4, lambda there: h1, g2, me, 1)
        if t in (2, 3, 4):
            y_from = lax.rem(y_lo + t - 1, 4)
            piece_to(x, y_from, {"dp_0": x_up}).wait_recv()
            piece_to(x, y_from, {"dp_0": x_up}).start()
            piece_to(x, y_from, {"dp_0": x_down}).start()
        if t == 3:
            gain_end(g2, 4, 1)
            h2[...] = total(g2, 4)
            g3[z] = h2[...]
            gain_hop(z_peer, slots, lambda there: h2, g3, z, 2)
        if t in (4, 5, 6):
            y_from = lax.rem(y_lo + t - 3, 4)
            piece_to(behind, y_from, {"dp_0": forward}).wait_recv()
            piece_to(behind, y_from, {"dp_0": forward}).start()

    gain_end(g3, slots, 2)
    h1_out = total(g3, slots)
    out_gain[dp] = h1_out
    gain_hop(dp_peer, 16, lambda there: out_gain.at[dp], out_gain, dp, 3)

    for q in range(cuts):
        hop_l(half - 1, q).wait_recv()
        hop_r(half - 1, q).wait_recv()
        cols_q = pl.ds(q * cut, cut)
        value = own(0, q) + in_l[half - 1, :, cols_q].astype(jnp.float32) + in_r[half - 1, :, cols_q].astype(jnp.float32)
        for k in range(4):
            give[k, :, cols_q] = value[2 * k : 2 * k + 2]

    def hand(k, _):
        there, to = quad_peer(k)
        remote(give.at[there], take.at[me], give_send, take_recv, to).start()
        return 0
    lax.fori_loop(1, 4, hand, 0)
    take[me] = give[me]

    for t in range(half):
        for q in range(cuts):
            if goes_l(t, q):
                hop_l(t, q).wait_send()
            if goes_r(t, q):
                hop_r(t, q).wait_send()
    for i in range(len(pieces)):
        beside(i).wait_send()
    for k in range(4):
        y_from = lax.rem(y_lo + k, 4)
        piece_to(forward, y_from, {"dp_0": forward}).wait_recv()
        piece_to(far, y_from, {"dp_0": forward}).wait_recv()
    await_bytes(pgh_all.at[pl.ds(0, 15)], all_send)
    to_side.wait_recv()
    to_side.wait_send()

    await_bytes(take.at[pl.ds(0, 3)], take_recv)
    await_bytes(give.at[pl.ds(0, 3)], give_send)
    out_ng[:, pl.ds(0, part)] = take[0] + take[2]
    out_ng[:, pl.ds(part, part)] = take[1] + take[3]
    gain_end(out_gain, 16, 3)
    for dst, n, stage in ((g1, 16, 0), (g2, 4, 1), (g3, slots, 2), (out_gain, 16, 3)):
        await_bytes(dst.at[pl.ds(0, n - 1)], gain_send.at[stage])


def exchange(ng, pgh, gp, cols):
    slots, _, width = ng.shape
    part, half = width // 2, slots // 2
    replicas, _, block = gp.shape
    dma = pltpu.SemaphoreType.DMA
    bf16, f32 = jnp.bfloat16, jnp.float32
    hops = (half, SUM_CUTS)
    line = pltpu.VMEM((half, 8, part), bf16)
    return pl.pallas_call(
        exchange_kernel,
        name="exchange",
        out_shape=(
            jax.ShapeDtypeStruct((2, width), f32),
            jax.ShapeDtypeStruct((replicas, *pgh.shape), bf16),
            jax.ShapeDtypeStruct(gp.shape, f32),
            jax.ShapeDtypeStruct(cols.shape, bf16),
        ),
        in_specs=[VMEM] * 4,
        out_specs=[VMEM] * 4,
        scratch_shapes=[
            pltpu.VMEM((slots, 8, part), bf16), line, line, line, line,
            pltpu.VMEM((4, 2, part), f32), pltpu.VMEM((4, 2, part), f32),
            pltpu.VMEM((16, 1, block), f32), pltpu.VMEM((4, 1, block), f32), pltpu.VMEM((slots, 1, block), f32),
            pltpu.VMEM((1, block), f32), pltpu.VMEM((1, block), f32),
            dma((5,)), dma((5,)), dma, dma, dma(hops), dma(hops), dma(hops), dma(hops),
            dma, dma, dma, dma((16,)), dma((4,)), dma((4,)),
        ],
        compiler_params=pltpu.CompilerParams(collective_id=2, has_side_effects=True),
    )(ng, pgh, gp, cols)


def gelu_value(preact):
    return 0.5 * preact * (1.0 + lax.erf(preact * 0.7071067811865476))


def gelu_slope(preact):
    return (
        0.5 * (1.0 + lax.erf(preact * 0.7071067811865476))
        + preact * jnp.exp(-0.5 * preact * preact) * 0.3989422804014327
    )


def contract_rows(left, right):
    return lax.dot_general(
        left, right, (((0,), (0,)), ((), ())), preferred_element_type=jnp.float32
    )


def contract_cols(left, right):
    return lax.dot_general(
        left, right, (((1,), (1,)), ((), ())), preferred_element_type=jnp.float32
    )


def swap_halves(rows):
    return jnp.roll(rows.reshape(-1, 8, rows.shape[1]), 4, axis=1).reshape(rows.shape)


def per_device(tokens, norm_gain, up_weight, down_weight, out_grad):
    slots, replicas = lax.axis_size("mp_0"), lax.axis_size(DP)
    width = tokens.shape[1]
    group = slots * 8
    ring, other, cols = gather_rows(tokens, out_grad, norm_gain[None], slots, replicas)

    own_first = lax.rem(lax.axis_index("mp_1") + lax.axis_index("mp_2"), 2) == 0
    pick = (lax.broadcasted_iota(jnp.int32, (1, 8, 1), 1) < 4) == own_first
    normed = jnp.where(pick, ring, other).reshape(group, width)
    cotan = jnp.where(pick, other, ring).reshape(group, width)

    preact = jnp.dot(normed, up_weight, preferred_element_type=jnp.float32)
    hid_grad = swap_halves(contract_cols(cotan, down_weight))
    hidden = swap_halves(gelu_value(preact)).astype(jnp.bfloat16)
    pre_grad = (hid_grad * gelu_slope(preact)).astype(jnp.bfloat16)
    partial = contract_cols(pre_grad, up_weight)
    gain_part = jnp.sum(partial * normed.astype(jnp.float32), axis=0)

    norm_grad, both_all, gain_sum, other_cols = exchange(
        partial.astype(jnp.bfloat16).reshape(slots, 8, width),
        jnp.stack([pre_grad, hidden]),
        gain_part.reshape(replicas, 1, width // replicas),
        cols,
    )

    factor = 1.0 / math.sqrt(group * replicas)
    gain_grad = gain_sum.reshape(width) / norm_gain * factor
    x_hat, inv_std = normalised(tokens)
    scaled = norm_gain * norm_grad
    input_grad = (
        scaled
        - jnp.mean(scaled, axis=1, keepdims=True)
        - x_hat * jnp.mean(scaled * x_hat, axis=1, keepdims=True)
    ) * inv_std

    pick = pick[None]
    block = width // replicas
    normed_cols = jnp.where(pick, cols, other_cols).reshape(-1, block)
    cotan_cols = jnp.where(pick, other_cols, cols).reshape(-1, block)
    pre_all = both_all[:, 0].reshape(-1, up_weight.shape[1])
    hid_all = both_all[:, 1].reshape(-1, up_weight.shape[1])
    up_grad = (contract_rows(normed_cols, pre_all) * factor).astype(jnp.bfloat16)
    down_grad = (contract_rows(hid_all, cotan_cols) * factor).astype(jnp.bfloat16)
    return (input_grad.astype(jnp.bfloat16), up_grad, down_grad, gain_grad)


def solution(mesh):
    torus = Mesh(mesh.devices.reshape(4, 4, 16, 2, 2), ("dp_0", "dp_1", "mp_0", "mp_1", "mp_2"))
    return jax.shard_map(
        per_device,
        mesh=torus,
        in_specs=(P(DP_MP, None), P(), P(None, MP), P(MP, None), P(DP_MP, None)),
        out_specs=(P(DP_MP, None), P(DP, MP), P(MP, DP), P()),
        check_vma=False,
    )
```
